32 devices in a mesh: half: 2 (over core), blk: 4 (over z), sub: 4 (over y, x).
Axes of the slice: x: 2, y: 2, z: 4, core: 2. Of those that a mesh axis runs over, the one named last changes fastest.
Arguments:
- leaf_expansions: float32 [16384, 128], P(('half', 'blk', 'sub')), may hold values from -0.3 to 0.3
- leaf_occupied: int32 [16384], P(('half', 'blk', 'sub')), may hold values 0 or 1
- cone_angles: float32 [2, 48], replicated, may hold values from -3.140625 to 3.140625
- cone_need3: int32 [48, 32], P(('half', 'blk'), 'sub'), may hold values 0 or 1
- cone_need4: int32 [48, 4], P(('half', 'blk'), 'sub'), may hold values 0 or 1
Outputs:
- lowfreq: float32 [256, 128], P(('half', 'blk', 'sub'))
- cone_expansions: float32 [48, 4, 128], P(('half', 'blk'), 'sub')
The draws below stay inside these ranges and needn't reach their ends.
All inputs are finite; a program needn't handle non-finite values. No bound on the sum of `leaf_occupied` or of `cone_need3` or of `cone_need4` on one device may be relied on, other than what follows from the above.
Results may differ from the reference program's by a relative error of at most 0.00007.
Values sent between devices are 32-bit elements; how exact they have to be, the bound alone decides.
A program may use at most 64 MiB of HBM per device.

```python
import math
import jax
import jax.numpy as jnp
from jax import lax

ORDER = 4
NODES = 64
CONE_DEV = 6
CONES = 48
LEAF_DEV = 512
LEAVES = 16384
BOX3 = 32
BOX4 = 4
N_HALF = 2
N_BLK = 4
N_SUB = 4


def touch_ends(values, stream_key, smallest, top_value):
    spot = [jax.random.randint(jax.random.fold_in(stream_key, axis), (), 0, length) for axis, length in enumerate(values.shape)]
    longest = values.shape.index(max(values.shape))
    neighbour = spot[:longest] + [(spot[longest] + 1) % values.shape[longest]] + spot[longest + 1:]
    return values.at[tuple(spot)].set(smallest).at[tuple(neighbour)].set(top_value)


def shard_levels(own_key, dims, shards, low, high):
    loudness, own = 1.0, jax.random.fold_in(own_key, 6)
    for dim, parts in shards:
        heights = jnp.exp(jax.random.uniform(jax.random.fold_in(own, dim), (parts,), jnp.float32, low / len(shards), high / len(shards)))
        loudness = loudness * jnp.repeat(heights, dims[dim] // parts).reshape([-1 if axis == dim else 1 for axis in range(len(dims))])
    return loudness


def scatter_about(rng, dims, deviation, most, shards=(), kind=jnp.bfloat16):
    values = deviation * jax.random.normal(rng, dims, jnp.float32)
    if shards:
        values = values * shard_levels(rng, dims, shards, -0.22, 0.18)
    return jnp.clip(values, -most, most).astype(kind)


def setup_inputs(seed: int = 0) -> dict:
    arg_keys = jax.random.split(jax.random.key(seed), 6)
    return {
        "leaf_expansions": scatter_about(arg_keys[0], (LEAVES, 2 * NODES), 0.05, 0.3, ((0, 32),), jnp.float32),
        "leaf_occupied": touch_ends((jax.random.randint(arg_keys[1], (LEAVES,), 0, 2) < 1).astype(jnp.int32), jax.random.fold_in(arg_keys[1], 1), 0, 1),
        "cone_angles": jnp.clip(jax.random.uniform(arg_keys[2], (2, CONES), jnp.float32, -3.140625, 3.140625), -3.140625, 3.140625),
        "cone_need3": touch_ends((jax.random.randint(arg_keys[3], (CONES, BOX3), 0, 4) < 3).astype(jnp.int32), jax.random.fold_in(arg_keys[3], 1), 0, 1),
        "cone_need4": touch_ends((jax.random.randint(arg_keys[4], (CONES, BOX4), 0, 4) < 3).astype(jnp.int32), jax.random.fold_in(arg_keys[4], 1), 0, 1),
    }


near_scale = 1.5
far_scale = 3.0
highest = lax.Precision.HIGHEST


def chebyshev_points(per_axis):
    index = jnp.arange(per_axis, dtype=jnp.float32)
    return jnp.cos((2.0 * index + 1.0) * math.pi / (2.0 * per_axis))


def octant_signs():
    octant = jnp.arange(8, dtype=jnp.int32)
    bits = jnp.stack([(octant // 4) % 2, (octant // 2) % 2, octant % 2], -1)
    return bits.astype(jnp.float32) * 2.0 - 1.0


def octant_table(per_axis):
    points = chebyshev_points(per_axis)
    degree = jnp.arange(1, per_axis, dtype=jnp.float32)
    sign_pair = jnp.array([-1.0, 1.0], dtype=jnp.float32)
    shifted = (points[None, :] + sign_pair[:, None]) / 2.0
    poly_here = jnp.cos(degree[None, :] * jnp.arccos(points)[:, None])
    poly_there = jnp.cos(degree[None, None, :] * jnp.arccos(shifted)[:, :, None])
    single = 1.0 / per_axis + (2.0 / per_axis) * jnp.einsum('mk,bnk->bmn', poly_here, poly_there, precision=highest)
    signs = octant_signs()
    along_x = jnp.where((signs[:, 0] > 0)[:, None, None], single[1][None], single[0][None])
    along_y = jnp.where((signs[:, 1] > 0)[:, None, None], single[1][None], single[0][None])
    along_z = jnp.where((signs[:, 2] > 0)[:, None, None], single[1][None], single[0][None])
    full = jnp.einsum('oad,obe,ocf->odefabc', along_x, along_y, along_z, precision=highest)
    node_count = per_axis ** 3
    return full.reshape(8, node_count, node_count)


def node_offsets(per_axis):
    points = chebyshev_points(per_axis)
    index = jnp.arange(per_axis ** 3, dtype=jnp.int32)
    coords = jnp.stack([points[index // (per_axis * per_axis)], points[(index // per_axis) % per_axis], points[index % per_axis]], -1)
    return coords[None, :, :] + octant_signs()[:, None, :]


def phases(angles, strength, per_axis):
    polar = angles[0]
    azimuth = angles[1]
    direction = jnp.stack([jnp.sin(polar) * jnp.cos(azimuth), jnp.sin(polar) * jnp.sin(azimuth), jnp.cos(polar)], -1)
    offsets = node_offsets(per_axis)
    argument = offsets[None, :, :, 0] * direction[:, None, None, 0]
    argument = argument + offsets[None, :, :, 1] * direction[:, None, None, 1]
    argument = argument + offsets[None, :, :, 2] * direction[:, None, None, 2]
    argument = -strength * argument
    return jnp.cos(argument), jnp.sin(argument)


def interpolate(real_part, imag_part, cosines, sine_part, transfer):
    mod_real = cosines * real_part - sine_part * imag_part
    mod_imag = cosines * imag_part + sine_part * real_part
    out_real = jnp.einsum('...on,onm->...m', mod_real, transfer, precision=highest)
    out_imag = jnp.einsum('...on,onm->...m', mod_imag, transfer, precision=highest)
    return out_real, out_imag


def reference(leaf_expansions, leaf_occupied, cone_angles, cone_need3, cone_need4):
    node_count = NODES
    groups = N_HALF * N_BLK
    level_one_count = LEAF_DEV // 8
    pair_count = level_one_count // 2
    per_sub = pair_count // N_SUB
    per_box = per_sub // 8
    transfer = octant_table(ORDER)
    masked = leaf_expansions * leaf_occupied.astype(jnp.float32)[:, None]
    masked = masked.reshape(groups, N_SUB, level_one_count, 8, 2, node_count)
    level_one = jnp.einsum('gspoan,onm->gspam', masked, transfer, precision=highest)
    level_one = level_one.reshape(groups, N_SUB, pair_count, 2, 2, node_count)
    level_one = jnp.transpose(level_one, (0, 2, 1, 3, 4, 5)).reshape(groups, pair_count, 2 * N_SUB, 2, node_count)
    level_two = jnp.einsum('gkoan,onm->gkam', level_one, transfer[:2 * N_SUB], precision=highest)
    lowfreq = level_two.reshape(groups * pair_count, 2 * node_count)
    box_rows = level_two.reshape(groups, N_SUB, per_box, 8, 2, node_count)
    box_rows = jnp.transpose(box_rows, (1, 0, 2, 3, 4, 5)).reshape(N_SUB * groups * per_box, 8, 2, node_count)
    real_part = box_rows[:, :, 0, :]
    imag_part = box_rows[:, :, 1, :]
    angle_blocks = jnp.transpose(cone_angles.reshape(2, groups, CONE_DEV), (1, 0, 2))
    need_three = cone_need3.reshape(groups, CONE_DEV, -1)
    need_four = cone_need4.reshape(groups, CONE_DEV, -1)

    def one_block(inputs):
        angles, mask_three, mask_four = inputs
        cos_near, sin_near = phases(angles, near_scale, ORDER)
        three_real, three_imag = interpolate(real_part[None], imag_part[None], cos_near[:, None], sin_near[:, None], transfer)
        weight = mask_three.astype(jnp.float32)[:, :, None]
        three_real = three_real * weight
        three_imag = three_imag * weight
        shape_six = (CONE_DEV, N_SUB, groups // 8, 8, per_box, node_count)
        three_real = jnp.transpose(three_real.reshape(shape_six), (0, 1, 2, 4, 3, 5)).reshape(CONE_DEV, -1, 8, node_count)
        three_imag = jnp.transpose(three_imag.reshape(shape_six), (0, 1, 2, 4, 3, 5)).reshape(CONE_DEV, -1, 8, node_count)
        cos_far, sin_far = phases(angles, far_scale, ORDER)
        four_real, four_imag = interpolate(three_real, three_imag, cos_far[:, None], sin_far[:, None], transfer)
        joined = jnp.concatenate([four_real, four_imag], -1)
        return joined * mask_four.astype(jnp.float32)[:, :, None]

    cone_expansions = lax.map(one_block, (angle_blocks, need_three, need_four))
    cone_expansions = cone_expansions.reshape(CONES, -1, 2 * node_count)
    return lowfreq, cone_expansions
```

```python
import functools
import math

import jax
import jax.numpy as jnp
import numpy as np
from jax import lax
from jax.experimental import pallas as pl
from jax.experimental.pallas import tpu as pltpu
from jax.sharding import PartitionSpec as P

MESH = pl.DeviceIdType.MESH
F32, BF16 = jnp.float32, jnp.bfloat16
ORDER = 4
OCT = 8
NEAR = 1.5


def octant_signs():
    octant = np.arange(OCT)
    return np.stack([octant // 4 % 2, octant // 2 % 2, octant % 2], -1) * 2.0 - 1.0


def chebyshev_points(per_axis):
    return np.cos((2.0 * np.arange(per_axis) + 1.0) * math.pi / (2.0 * per_axis))


def octant_table(per_axis):
    points = chebyshev_points(per_axis)
    degree = np.arange(1, per_axis)
    shifted = (points[None, :] + np.array([-1.0, 1.0])[:, None]) / 2.0
    here = np.cos(degree[None, :] * np.arccos(points)[:, None])
    there = np.cos(degree * np.arccos(shifted)[:, :, None])
    single = 1.0 / per_axis + 2.0 / per_axis * np.einsum("mk,bnk->bnm", here, there)
    bit = (octant_signs() > 0).astype(int)
    full = np.einsum("oda,oeb,ofc->odefabc", single[bit[:, 0]], single[bit[:, 1]], single[bit[:, 2]])
    return full.reshape(OCT, per_axis**3, per_axis**3)


def weight_table(per_axis):
    table = octant_table(per_axis).astype(np.float32)
    nodes = per_axis**3
    wide = np.zeros((OCT, 2, nodes, 2, nodes), np.float32)
    wide[:, 0, :, 0, :] = table
    wide[:, 1, :, 1, :] = table
    wide = wide.reshape(OCT * 2 * nodes, 2 * nodes)
    high = wide.astype(BF16)
    low = (wide - high.astype(np.float32)).astype(BF16)
    return np.concatenate([high, low], 1)


def lane_table(per_axis):
    points = chebyshev_points(per_axis)
    index = np.arange(per_axis**3)
    coords = np.stack([points[index // per_axis**2], points[index // per_axis % per_axis], points[index % per_axis]])
    offsets = coords[:, None, :] + octant_signs().T[:, :, None]
    offsets = -NEAR * np.concatenate([offsets, offsets], -1).reshape(3, -1)
    sign = np.tile(np.repeat([-1.0, 1.0], per_axis**3), OCT)
    return np.concatenate([offsets, sign[None]], 0).astype(np.float32)


def each(count, body):
    if count <= 16:
        for d in range(1, count):
            body(d)
    else:
        lax.fori_loop(1, count, lambda d, c: (body(d), c)[1], 0)


def split_rows(value):
    high = value.astype(BF16)
    low = (value - high.astype(F32)).astype(BF16)
    return jnp.concatenate([high, low], 0)


def fold(acc, rows, width):
    return (acc[:rows, :width] + acc[rows:, :width]) + (acc[:rows, width:] + acc[rows:, width:])


def kernel(
    halves, blks, subs, cones,
    leaf_hbm, occ_hbm, angle_hbm, need3_hbm, need4_hbm, weight_hbm, lane_hbm,
    low_out, cone_out,
    leaf, occ, angle, need3, need4, weight, lane, part, got, low, phase,
    in_sem, send1, recv1, send2, recv2,
):
    groups = halves * blks
    half, blk, sub = lax.axis_index("half"), lax.axis_index("blk"), lax.axis_index("sub")
    group = half * blks + blk
    rows, width = leaf.shape
    pairs = rows // (2 * OCT)
    per_sub = pairs // subs

    loads = [
        pltpu.make_async_copy(src, dst, in_sem.at[i])
        for i, (src, dst) in enumerate([
            (occ_hbm, occ), (leaf_hbm, leaf), (weight_hbm, weight), (angle_hbm, angle),
            (lane_hbm, lane), (need3_hbm, need3), (need4_hbm, need4),
        ])
    ]
    for load in loads:
        load.start()

    def sub_peer(d):
        return {"sub": lax.rem(sub + d, subs)}

    def group_peer(d):
        peer = lax.rem(group + d, groups)
        return {"half": peer // blks, "blk": lax.rem(peer, blks)}

    barrier = pltpu.get_barrier_semaphore()

    def greet(peer, d):
        pl.semaphore_signal(barrier, inc=1, device_id=peer(d), device_id_type=MESH)

    each(groups, functools.partial(greet, group_peer))
    each(subs, functools.partial(greet, sub_peer))

    loads[0].wait()
    loads[1].wait()
    columns = jnp.transpose(occ[...].astype(F32))
    for i in range(rows // 128):
        chunk = pl.ds(i * 128, 128)
        leaf[chunk, :] = leaf[chunk, :] * columns[:, i : i + 1]
    loads[2].wait()
    acc = None
    for t in range(OCT // 2):
        tile = jnp.concatenate(
            [
                jnp.concatenate(
                    [leaf[pl.ds(OCT * r + o, pairs, stride=2 * OCT), :] for o in (2 * t, 2 * t + 1)], 1
                )
                for r in range(2)
            ],
            0,
        )
        term = jnp.dot(
            split_rows(tile), weight[2 * width * t : 2 * width * (t + 1), :], preferred_element_type=F32
        )
        acc = term if acc is None else acc + term
    one = fold(acc, 2 * pairs, width)
    tile = jnp.concatenate([one[:pairs], one[pairs:]], 1)
    mine = weight[pl.ds(pl.multiple_of(sub * 2 * width, 2 * width), 2 * width), :]
    part[...] = fold(jnp.dot(split_rows(tile), mine, preferred_element_type=F32), pairs, width)

    pl.semaphore_wait(barrier, (groups - 1) + (subs - 1))

    def rows_of(index):
        return pl.ds(pl.multiple_of(index * per_sub, 8), per_sub)

    def copy_one(d):
        return pltpu.make_async_remote_copy(
            src_ref=part.at[rows_of(lax.rem(sub + d, subs))],
            dst_ref=got.at[d],
            send_sem=send1.at[d],
            recv_sem=recv1.at[d],
            device_id=sub_peer(d),
            device_id_type=MESH,
        )

    each(subs, lambda d: copy_one(d).start())

    loads[3].wait()
    loads[4].wait()
    padded = phase.shape[1]
    count = angle.shape[1]
    pick = lax.broadcasted_iota(jnp.int32, (padded, count), 1) == (
        lax.broadcasted_iota(jnp.int32, (padded, count), 0) + group * cones
    )
    polar = jnp.sum(jnp.where(pick, angle[0:1, :], 0.0), 1, keepdims=True)
    azimuth = jnp.sum(jnp.where(pick, angle[1:2, :], 0.0), 1, keepdims=True)
    sin_polar = jnp.sin(polar)
    argument = (
        (sin_polar * jnp.cos(azimuth)) * lane[0:1, :]
        + (sin_polar * jnp.sin(azimuth)) * lane[1:2, :]
        + jnp.cos(polar) * lane[2:3, :]
    )
    cosine, sine = jnp.cos(argument), jnp.sin(argument)
    sign = lane[3:4, :]
    phase[0] = cosine
    phase[1] = sine * sign
    phase[2] = 1.0 - 2.0 * sine * sine
    phase[3] = 2.0 * sine * cosine * sign
    loads[5].wait()
    loads[6].wait()

    each(subs, lambda d: copy_one(d).wait())
    total = part[rows_of(sub), :]
    for d in range(1, subs):
        total = total + got[d]
    low[group] = total
    low_out[...] = total

    def copy_two(d):
        return pltpu.make_async_remote_copy(
            src_ref=low.at[group],
            dst_ref=low.at[group],
            send_sem=send2.at[d],
            recv_sem=recv2.at[d],
            device_id=group_peer(d),
            device_id_type=MESH,
        )

    each(groups, lambda d: copy_two(d).start())
    each(groups, lambda d: copy_two(d).wait())

    def widen(value):
        fill = padded - cones
        if fill:
            value = jnp.concatenate([value, jnp.zeros((fill, value.shape[1]), value.dtype)], 0)
        return value.astype(F32)

    keep3 = widen(need3[...])
    lanes4 = need4.shape[1]
    diagonal = lax.broadcasted_iota(jnp.int32, (padded, lanes4), 0) == lax.broadcasted_iota(
        jnp.int32, (padded, lanes4), 1
    )

    def product(pieces):
        rows_in = pieces[0].shape[0]
        acc = None
        for t in range(OCT // 2):
            tile = split_rows(jnp.concatenate(pieces[2 * t : 2 * t + 2], 1))
            term = jnp.dot(tile, weight[2 * width * t : 2 * width * (t + 1), :], preferred_element_type=F32)
            acc = term if acc is None else acc + term
        return fold(acc, rows_in, width)

    for q in range(groups // OCT):
        boxes = [low[q * OCT + g] for g in range(OCT)]
        turned = [pltpu.roll(box, width // 2, 1) for box in boxes]
        pieces = []
        for o in range(OCT):
            lanes = slice(o * width, (o + 1) * width)
            cos_o, sin_o = phase[0, :, lanes], phase[1, :, lanes]
            pieces.append(
                jnp.concatenate(
                    [cos_o * boxes[g][o : o + 1, :] + sin_o * turned[g][o : o + 1, :] for g in range(OCT)], 0
                )
            )
        three = product(pieces)
        pieces = []
        for o in range(OCT):
            lanes = slice(o * width, (o + 1) * width)
            column = q * OCT + o
            box = three[o * padded : (o + 1) * padded] * keep3[:, column : column + 1]
            pieces.append(phase[2, :, lanes] * box + phase[3, :, lanes] * pltpu.roll(box, width // 2, 1))
        keep4 = jnp.sum(jnp.where(diagonal, need4[q : q + 1, :].astype(F32), 0.0), 1, keepdims=True)
        four = product(pieces) * keep4
        cone_out[:, q, :] = four[:cones]


def solution(mesh):
    halves, blks, subs = mesh.shape["half"], mesh.shape["blk"], mesh.shape["sub"]
    groups = halves * blks

    def local(leaf, occupied, angles, need3, need4):
        rows, width = leaf.shape
        pairs = rows // (2 * OCT)
        per_sub = pairs // subs
        cones = need3.shape[0]
        padded = -(-cones // 8) * 8
        assert per_sub == OCT and need3.shape[1] == groups
        weight = jnp.asarray(weight_table(ORDER))
        lane = jnp.asarray(lane_table(ORDER))
        occupied = occupied.reshape(rows // 128, 128)
        need4 = need4.T
        vmem = pl.BlockSpec(memory_space=pltpu.VMEM)
        anywhere = pl.BlockSpec(memory_space=pl.ANY)
        return pl.pallas_call(
            functools.partial(kernel, halves, blks, subs, cones),
            out_shape=(
                jax.ShapeDtypeStruct((per_sub, width), F32),
                jax.ShapeDtypeStruct((cones, groups // OCT, width), F32),
            ),
            in_specs=[anywhere] * 7,
            out_specs=(vmem, vmem),
            scratch_shapes=[
                pltpu.VMEM(leaf.shape, F32),
                pltpu.VMEM(occupied.shape, jnp.int32),
                pltpu.VMEM(angles.shape, F32),
                pltpu.VMEM(need3.shape, jnp.int32),
                pltpu.VMEM(need4.shape, jnp.int32),
                pltpu.VMEM(weight.shape, BF16),
                pltpu.VMEM(lane.shape, F32),
                pltpu.VMEM((pairs, width), F32),
                pltpu.VMEM((subs, per_sub, width), F32),
                pltpu.VMEM((groups, per_sub, width), F32),
                pltpu.VMEM((4, padded, OCT * width), F32),
                pltpu.SemaphoreType.DMA((7,)),
                pltpu.SemaphoreType.DMA((subs,)),
                pltpu.SemaphoreType.DMA((subs,)),
                pltpu.SemaphoreType.DMA((groups,)),
                pltpu.SemaphoreType.DMA((groups,)),
            ],
            compiler_params=pltpu.CompilerParams(collective_id=0, has_side_effects=True),
            name="upward",
        )(leaf, occupied, angles, need3, need4, weight, lane)

    return jax.shard_map(
        local,
        mesh=mesh,
        in_specs=(
            P(("half", "blk", "sub"), None),
            P(("half", "blk", "sub")),
            P(),
            P(("half", "blk"), "sub"),
            P(("half", "blk"), "sub"),
        ),
        out_specs=(P(("half", "blk", "sub"), None), P(("half", "blk"), "sub", None)),
        check_vma=False,
    )
```

```python
import functools
import math

import jax
import jax.numpy as jnp
import numpy as np
from jax import lax
from jax.experimental import pallas as pl
from jax.experimental.pallas import tpu as pltpu
from jax.sharding import PartitionSpec as P

MESH = pl.DeviceIdType.MESH
F32, BF16 = jnp.float32, jnp.bfloat16
ORDER = 4
OCT = 8
NEAR = 1.5


def octant_signs():
    octant = np.arange(OCT)
    return np.stack([octant // 4 % 2, octant // 2 % 2, octant % 2], -1) * 2.0 - 1.0


def chebyshev_points(per_axis):
    return np.cos((2.0 * np.arange(per_axis) + 1.0) * math.pi / (2.0 * per_axis))


def octant_table(per_axis):
    points = chebyshev_points(per_axis)
    degree = np.arange(1, per_axis)
    shifted = (points[None, :] + np.array([-1.0, 1.0])[:, None]) / 2.0
    here = np.cos(degree[None, :] * np.arccos(points)[:, None])
    there = np.cos(degree * np.arccos(shifted)[:, :, None])
    single = 1.0 / per_axis + 2.0 / per_axis * np.einsum("mk,bnk->bnm", here, there)
    bit = (octant_signs() > 0).astype(int)
    full = np.einsum("oda,oeb,ofc->odefabc", single[bit[:, 0]], single[bit[:, 1]], single[bit[:, 2]])
    return full.reshape(OCT, per_axis**3, per_axis**3)


def weight_table(per_axis):
    table = octant_table(per_axis).astype(np.float32)
    nodes = per_axis**3
    wide = np.zeros((OCT, 2, nodes, 2, nodes), np.float32)
    wide[:, 0, :, 0, :] = table
    wide[:, 1, :, 1, :] = table
    wide = wide.reshape(OCT * 2 * nodes, 2 * nodes)
    high = wide.astype(BF16)
    low = (wide - high.astype(np.float32)).astype(BF16)
    return np.concatenate([high, low], 1)


def lane_table(per_axis):
    points = chebyshev_points(per_axis)
    index = np.arange(per_axis**3)
    coords = np.stack([points[index // per_axis**2], points[index // per_axis % per_axis], points[index % per_axis]])
    offsets = coords[:, None, :] + octant_signs().T[:, :, None]
    offsets = -NEAR * np.concatenate([offsets, offsets], -1).reshape(3, -1)
    sign = np.tile(np.repeat([-1.0, 1.0], per_axis**3), OCT)
    return np.concatenate([offsets, sign[None]], 0).astype(np.float32)


def each(count, body):
    if count <= 64:
        for d in range(1, count):
            body(d)
    else:
        lax.fori_loop(1, count, lambda d, c: (body(d), c)[1], 0)


def split_rows(value):
    high = value.astype(BF16)
    low = (value - high.astype(F32)).astype(BF16)
    return jnp.concatenate([high, low], 0)


def fold(acc, rows, width):
    return (acc[:rows, :width] + acc[rows:, :width]) + (acc[:rows, width:] + acc[rows:, width:])


def kernel(
    halves, blks, subs, cones,
    leaf_hbm, occ_hbm, angle_hbm, need3_hbm, need4_hbm, weight_hbm, lane_hbm,
    low_out, cone_out,
    leaf, occ, angle, need3, need4, weight, lane, part, got, low, phase,
    in_sem, send, recv, send2, recv2,
):
    groups = halves * blks
    half, blk, sub = lax.axis_index("half"), lax.axis_index("blk"), lax.axis_index("sub")
    group = half * blks + blk
    rows, width = leaf.shape
    pairs = rows // (2 * OCT)
    per_sub = pairs // subs

    loads = [
        pltpu.make_async_copy(src, dst, in_sem.at[i])
        for i, (src, dst) in enumerate([
            (occ_hbm, occ), (leaf_hbm, leaf), (weight_hbm, weight), (angle_hbm, angle),
            (lane_hbm, lane), (need3_hbm, need3), (need4_hbm, need4),
        ])
    ]
    for load in loads:
        load.start()

    def peer(d):
        there = lax.rem(blk + d // subs, blks)
        return {"blk": there, "sub": lax.rem(sub + lax.rem(d, subs), subs)}

    def half_peer(e):
        return {"half": lax.rem(half + e, halves)}

    barrier = pltpu.get_barrier_semaphore()

    def greet(target):
        pl.semaphore_signal(barrier, inc=1, device_id=target, device_id_type=MESH)

    each(halves, lambda e: greet(half_peer(e)))
    each(blks * subs, lambda d: greet(peer(d)))

    loads[0].wait()
    loads[1].wait()
    columns = jnp.transpose(occ[...].astype(F32))
    for i in range(rows // 128):
        chunk = pl.ds(i * 128, 128)
        leaf[chunk, :] = leaf[chunk, :] * columns[:, i : i + 1]
    loads[2].wait()
    acc = None
    for t in range(OCT // 2):
        tile = jnp.concatenate(
            [
                jnp.concatenate(
                    [leaf[pl.ds(OCT * r + o, pairs, stride=2 * OCT), :] for o in (2 * t, 2 * t + 1)], 1
                )
                for r in range(2)
            ],
            0,
        )
        term = jnp.dot(
            split_rows(tile), weight[2 * width * t : 2 * width * (t + 1), :], preferred_element_type=F32
        )
        acc = term if acc is None else acc + term
    one = fold(acc, 2 * pairs, width)
    tile = jnp.concatenate([one[:pairs], one[pairs:]], 1)
    mine = weight[pl.ds(pl.multiple_of(sub * 2 * width, 2 * width), 2 * width), :]
    part[...] = fold(jnp.dot(split_rows(tile), mine, preferred_element_type=F32), pairs, width)

    pl.semaphore_wait(barrier, blks * subs + halves - 2)

    def rows_of(index):
        return pl.ds(pl.multiple_of(index * per_sub, 8), per_sub)

    def copy(d):
        return pltpu.make_async_remote_copy(
            src_ref=part.at[rows_of(lax.rem(sub + lax.rem(d, subs), subs))],
            dst_ref=got.at[blk, sub],
            send_sem=send.at[d],
            recv_sem=recv.at[d],
            device_id=peer(d),
            device_id_type=MESH,
        )

    each(blks * subs, lambda d: copy(d).start())
    got[blk, sub] = part[rows_of(sub), :]

    loads[3].wait()
    loads[4].wait()
    padded = phase.shape[1]
    count = angle.shape[1]
    pick = lax.broadcasted_iota(jnp.int32, (padded, count), 1) == (
        lax.broadcasted_iota(jnp.int32, (padded, count), 0) + group * cones
    )
    polar = jnp.sum(jnp.where(pick, angle[0:1, :], 0.0), 1, keepdims=True)
    azimuth = jnp.sum(jnp.where(pick, angle[1:2, :], 0.0), 1, keepdims=True)
    sin_polar = jnp.sin(polar)
    argument = (
        (sin_polar * jnp.cos(azimuth)) * lane[0:1, :]
        + (sin_polar * jnp.sin(azimuth)) * lane[1:2, :]
        + jnp.cos(polar) * lane[2:3, :]
    )
    cosine, sine = jnp.cos(argument), jnp.sin(argument)
    sign = lane[3:4, :]
    phase[0] = cosine
    phase[1] = sine * sign
    phase[2] = 1.0 - 2.0 * sine * sine
    phase[3] = 2.0 * sine * cosine * sign
    loads[5].wait()
    loads[6].wait()

    def forward(index, e):
        there = half * blks + index
        return pltpu.make_async_remote_copy(
            src_ref=low.at[there],
            dst_ref=low.at[there],
            send_sem=send2.at[index, e],
            recv_sem=recv2.at[index, e],
            device_id=half_peer(e),
            device_id_type=MESH,
        )

    for step in range(blks):
        for t in range(subs):
            d = step * subs + t
            if d:
                copy(d).wait()
        there = lax.rem(blk + (blks - step) % blks, blks)
        total = functools.reduce(jnp.add, [got[there, t] for t in range(subs)])
        low[half * blks + there] = total
        if step == 0:
            low_out[...] = total
        each(halves, lambda e: forward(there, e).start())
    for step in range(blks):
        each(halves, lambda e: forward(lax.rem(blk + step, blks), e).wait())

    def widen(value):
        fill = padded - cones
        if fill:
            value = jnp.concatenate([value, jnp.zeros((fill, value.shape[1]), value.dtype)], 0)
        return value.astype(F32)

    keep3 = widen(need3[...])
    lanes4 = need4.shape[1]
    diagonal = lax.broadcasted_iota(jnp.int32, (padded, lanes4), 0) == lax.broadcasted_iota(
        jnp.int32, (padded, lanes4), 1
    )

    def product(pieces):
        rows_in = pieces[0].shape[0]
        acc = None
        for t in range(OCT // 2):
            tile = split_rows(jnp.concatenate(pieces[2 * t : 2 * t + 2], 1))
            term = jnp.dot(tile, weight[2 * width * t : 2 * width * (t + 1), :], preferred_element_type=F32)
            acc = term if acc is None else acc + term
        return fold(acc, rows_in, width)

    for q in range(groups // OCT):
        boxes = [low[q * OCT + g] for g in range(OCT)]
        turned = [pltpu.roll(box, width // 2, 1) for box in boxes]
        pieces = []
        for o in range(OCT):
            lanes = slice(o * width, (o + 1) * width)
            cos_o, sin_o = phase[0, :, lanes], phase[1, :, lanes]
            pieces.append(
                jnp.concatenate(
                    [cos_o * boxes[g][o : o + 1, :] + sin_o * turned[g][o : o + 1, :] for g in range(OCT)], 0
                )
            )
        three = product(pieces)
        pieces = []
        for o in range(OCT):
            lanes = slice(o * width, (o + 1) * width)
            column = q * OCT + o
            box = three[o * padded : (o + 1) * padded] * keep3[:, column : column + 1]
            pieces.append(phase[2, :, lanes] * box + phase[3, :, lanes] * pltpu.roll(box, width // 2, 1))
        keep4 = jnp.sum(jnp.where(diagonal, need4[q : q + 1, :].astype(F32), 0.0), 1, keepdims=True)
        four = product(pieces) * keep4
        cone_out[:, q, :] = four[:cones]


def put_out(low_ref, cone_ref, low_out, cone_out, sems):
    copies = [
        pltpu.make_async_copy(low_ref, low_out, sems.at[0]),
        pltpu.make_async_copy(cone_ref, cone_out, sems.at[1]),
    ]
    for copy in copies:
        copy.start()
    for copy in copies:
        copy.wait()


def solution(mesh):
    halves, blks, subs = mesh.shape["half"], mesh.shape["blk"], mesh.shape["sub"]
    groups = halves * blks

    def local(leaf, occupied, angles, need3, need4):
        rows, width = leaf.shape
        pairs = rows // (2 * OCT)
        per_sub = pairs // subs
        cones = need3.shape[0]
        padded = -(-cones // 8) * 8
        assert per_sub == OCT and need3.shape[1] == groups
        weight = jnp.asarray(weight_table(ORDER))
        lane = jnp.asarray(lane_table(ORDER))
        occupied = occupied.reshape(rows // 128, 128)
        need4 = need4.T
        vmem = pl.BlockSpec(memory_space=pltpu.VMEM)
        anywhere = pl.BlockSpec(memory_space=pl.ANY)
        results = pl.pallas_call(
            functools.partial(kernel, halves, blks, subs, cones),
            out_shape=(
                pltpu.VMEM((per_sub, width), F32),
                pltpu.VMEM((cones, groups // OCT, width), F32),
            ),
            in_specs=[anywhere] * 7,
            out_specs=(vmem, vmem),
            scratch_shapes=[
                pltpu.VMEM(leaf.shape, F32),
                pltpu.VMEM(occupied.shape, jnp.int32),
                pltpu.VMEM(angles.shape, F32),
                pltpu.VMEM(need3.shape, jnp.int32),
                pltpu.VMEM(need4.shape, jnp.int32),
                pltpu.VMEM(weight.shape, BF16),
                pltpu.VMEM(lane.shape, F32),
                pltpu.VMEM((pairs, width), F32),
                pltpu.VMEM((blks, subs, per_sub, width), F32),
                pltpu.VMEM((groups, per_sub, width), F32),
                pltpu.VMEM((4, padded, OCT * width), F32),
                pltpu.SemaphoreType.DMA((7,)),
                pltpu.SemaphoreType.DMA((blks * subs,)),
                pltpu.SemaphoreType.DMA((blks * subs,)),
                pltpu.SemaphoreType.DMA((blks, halves)),
                pltpu.SemaphoreType.DMA((blks, halves)),
            ],
            compiler_params=pltpu.CompilerParams(collective_id=0, has_side_effects=True),
            name="upward",
        )(leaf, occupied, angles, need3, need4, weight, lane)
        results = [pltpu.with_memory_space_constraint(value, pltpu.VMEM) for value in results]
        return pl.pallas_call(
            put_out,
            out_shape=[jax.ShapeDtypeStruct(value.shape, F32) for value in results],
            in_specs=[vmem] * 2,
            out_specs=[pl.BlockSpec(memory_space=pltpu.HBM)] * 2,
            scratch_shapes=[pltpu.SemaphoreType.DMA((2,))],
            name="put_out",
        )(*results)

    return jax.shard_map(
        local,
        mesh=mesh,
        in_specs=(
            P(("half", "blk", "sub"), None),
            P(("half", "blk", "sub")),
            P(),
            P(("half", "blk"), "sub"),
            P(("half", "blk"), "sub"),
        ),
        out_specs=(P(("half", "blk", "sub"), None), P(("half", "blk"), "sub", None)),
        check_vma=False,
    )
```

```python
import functools
import math

import jax
import jax.numpy as jnp
import numpy as np
from jax import lax
from jax.experimental import pallas as pl
from jax.experimental.pallas import tpu as pltpu
from jax.sharding import PartitionSpec as P

MESH = pl.DeviceIdType.MESH
F32, BF16 = jnp.float32, jnp.bfloat16
ORDER = 4
OCT = 8
NEAR = 1.5


def octant_signs():
    octant = np.arange(OCT)
    return np.stack([octant // 4 % 2, octant // 2 % 2, octant % 2], -1) * 2.0 - 1.0


def chebyshev_points(per_axis):
    return np.cos((2.0 * np.arange(per_axis) + 1.0) * math.pi / (2.0 * per_axis))


def octant_table(per_axis):
    points = chebyshev_points(per_axis)
    degree = np.arange(1, per_axis)
    shifted = (points[None, :] + np.array([-1.0, 1.0])[:, None]) / 2.0
    here = np.cos(degree[None, :] * np.arccos(points)[:, None])
    there = np.cos(degree * np.arccos(shifted)[:, :, None])
    single = 1.0 / per_axis + 2.0 / per_axis * np.einsum("mk,bnk->bnm", here, there)
    bit = (octant_signs() > 0).astype(int)
    full = np.einsum("oda,oeb,ofc->odefabc", single[bit[:, 0]], single[bit[:, 1]], single[bit[:, 2]])
    return full.reshape(OCT, per_axis**3, per_axis**3)


def weight_table(per_axis):
    table = octant_table(per_axis).astype(np.float32)
    nodes = per_axis**3
    wide = np.zeros((OCT, 2, nodes, 2, nodes), np.float32)
    wide[:, 0, :, 0, :] = table
    wide[:, 1, :, 1, :] = table
    wide = wide.reshape(OCT * 2 * nodes, 2 * nodes)
    high = wide.astype(BF16)
    low = (wide - high.astype(np.float32)).astype(BF16)
    return np.concatenate([high, low], 1)


def lane_table(per_axis):
    points = chebyshev_points(per_axis)
    index = np.arange(per_axis**3)
    coords = np.stack([points[index // per_axis**2], points[index // per_axis % per_axis], points[index % per_axis]])
    offsets = coords[:, None, :] + octant_signs().T[:, :, None]
    offsets = -NEAR * np.concatenate([offsets, offsets], -1).reshape(3, -1)
    sign = np.tile(np.repeat([-1.0, 1.0], per_axis**3), OCT)
    return np.concatenate([offsets, sign[None]], 0).astype(np.float32)


def each(count, body):
    if count <= 64:
        for d in range(1, count):
            body(d)
    else:
        lax.fori_loop(1, count, lambda d, c: (body(d), c)[1], 0)


def split_rows(value):
    high = value.astype(BF16)
    low = (value - high.astype(F32)).astype(BF16)
    return jnp.concatenate([high, low], 0)


def fold(acc, rows, width):
    return (acc[:rows, :width] + acc[rows:, :width]) + (acc[:rows, width:] + acc[rows:, width:])


def kernel(
    halves, blks, subs, cones,
    leaf_hbm, occ_hbm, angle_hbm, need3_hbm, need4_hbm, weight_hbm, lane_hbm,
    low_out, cone_out,
    leaf, occ, angle, need3, need4, weight, lane, part, got, low, three, phase,
    in_sem, send, recv, send2, recv2,
):
    groups = halves * blks
    half, blk, sub = lax.axis_index("half"), lax.axis_index("blk"), lax.axis_index("sub")
    group = half * blks + blk
    rows, width = leaf.shape
    pairs = rows // (2 * OCT)
    per_sub = pairs // subs

    loads = [
        pltpu.make_async_copy(src, dst, in_sem.at[i])
        for i, (src, dst) in enumerate([
            (occ_hbm, occ), (leaf_hbm, leaf), (weight_hbm, weight), (angle_hbm, angle),
            (lane_hbm, lane), (need3_hbm, need3), (need4_hbm, need4),
        ])
    ]
    for load in loads:
        load.start()

    def peer(d):
        there = lax.rem(blk + d // subs, blks)
        return {"blk": there, "sub": lax.rem(sub + lax.rem(d, subs), subs)}

    def half_peer(e):
        return {"half": lax.rem(half + e, halves)}

    barrier = pltpu.get_barrier_semaphore()

    def greet(target):
        pl.semaphore_signal(barrier, inc=1, device_id=target, device_id_type=MESH)

    each(halves, lambda e: greet(half_peer(e)))
    each(blks * subs, lambda d: greet(peer(d)))

    loads[0].wait()
    loads[1].wait()
    columns = jnp.transpose(occ[...].astype(F32))
    for i in range(rows // 128):
        chunk = pl.ds(i * 128, 128)
        leaf[chunk, :] = leaf[chunk, :] * columns[:, i : i + 1]
    loads[2].wait()
    acc = None
    for t in range(OCT // 2):
        tile = jnp.concatenate(
            [
                jnp.concatenate(
                    [leaf[pl.ds(OCT * r + o, pairs, stride=2 * OCT), :] for o in (2 * t, 2 * t + 1)], 1
                )
                for r in range(2)
            ],
            0,
        )
        term = jnp.dot(
            split_rows(tile), weight[2 * width * t : 2 * width * (t + 1), :], preferred_element_type=F32
        )
        acc = term if acc is None else acc + term
    one = fold(acc, 2 * pairs, width)
    tile = jnp.concatenate([one[:pairs], one[pairs:]], 1)
    mine = weight[pl.ds(pl.multiple_of(sub * 2 * width, 2 * width), 2 * width), :]
    part[...] = fold(jnp.dot(split_rows(tile), mine, preferred_element_type=F32), pairs, width)

    pl.semaphore_wait(barrier, blks * subs + halves - 2)

    def rows_of(index):
        return pl.ds(pl.multiple_of(index * per_sub, 8), per_sub)

    def copy(d):
        return pltpu.make_async_remote_copy(
            src_ref=part.at[rows_of(lax.rem(sub + lax.rem(d, subs), subs))],
            dst_ref=got.at[blk, sub],
            send_sem=send.at[d],
            recv_sem=recv.at[d],
            device_id=peer(d),
            device_id_type=MESH,
        )

    each(blks * subs, lambda d: copy(d).start())
    got[blk, sub] = part[rows_of(sub), :]

    loads[3].wait()
    loads[4].wait()
    padded = phase.shape[1]
    count = angle.shape[1]
    pick = lax.broadcasted_iota(jnp.int32, (padded, count), 1) == (
        lax.broadcasted_iota(jnp.int32, (padded, count), 0) + group * cones
    )
    polar = jnp.sum(jnp.where(pick, angle[0:1, :], 0.0), 1, keepdims=True)
    azimuth = jnp.sum(jnp.where(pick, angle[1:2, :], 0.0), 1, keepdims=True)
    sin_polar = jnp.sin(polar)
    argument = (
        (sin_polar * jnp.cos(azimuth)) * lane[0:1, :]
        + (sin_polar * jnp.sin(azimuth)) * lane[1:2, :]
        + jnp.cos(polar) * lane[2:3, :]
    )
    cosine, sine = jnp.cos(argument), jnp.sin(argument)
    sign = lane[3:4, :]
    phase[0] = cosine
    phase[1] = sine * sign
    phase[2] = 1.0 - 2.0 * sine * sine
    phase[3] = 2.0 * sine * cosine * sign
    loads[5].wait()
    loads[6].wait()

    def forward(index, e):
        there = half * blks + index
        return pltpu.make_async_remote_copy(
            src_ref=low.at[there],
            dst_ref=low.at[there],
            send_sem=send2.at[index, e],
            recv_sem=recv2.at[index, e],
            device_id=half_peer(e),
            device_id_type=MESH,
        )

    for step in range(blks):
        for t in range(subs):
            d = step * subs + t
            if d:
                copy(d).wait_recv()
        there = lax.rem(blk + (blks - step) % blks, blks)
        total = functools.reduce(jnp.add, [got[there, t] for t in range(subs)])
        low[half * blks + there] = total
        if step == 0:
            low_out[...] = total
        each(halves, lambda e: forward(there, e).start())
    def widen(value):
        fill = padded - cones
        if fill:
            value = jnp.concatenate([value, jnp.zeros((fill, value.shape[1]), value.dtype)], 0)
        return value.astype(F32)

    keep3 = widen(need3[...])
    lanes4 = need4.shape[1]
    diagonal = lax.broadcasted_iota(jnp.int32, (padded, lanes4), 0) == lax.broadcasted_iota(
        jnp.int32, (padded, lanes4), 1
    )

    def product(pieces):
        rows_in = pieces[0].shape[0]
        acc = None
        for t in range(OCT // 2):
            tile = split_rows(jnp.concatenate(pieces[2 * t : 2 * t + 2], 1))
            term = jnp.dot(tile, weight[2 * width * t : 2 * width * (t + 1), :], preferred_element_type=F32)
            acc = term if acc is None else acc + term
        return fold(acc, rows_in, width)

    def level_three(first):
        size = min(blks, OCT)
        for start in range(0, blks, size):
            boxes = [low[first + start + g] for g in range(size)]
            turned = [pltpu.roll(box, width // 2, 1) for box in boxes]
            pieces = []
            for o in range(OCT):
                lanes = slice(o * width, (o + 1) * width)
                cos_o, sin_o = phase[0, :, lanes], phase[1, :, lanes]
                pieces.append(
                    jnp.concatenate(
                        [cos_o * boxes[g][o : o + 1, :] + sin_o * turned[g][o : o + 1, :] for g in range(size)], 0
                    )
                )
            result = product(pieces)
            for g in range(size):
                three[first + start + g] = result[g * padded : (g + 1) * padded]

    level_three(half * blks)
    for step in range(blks):
        each(halves, lambda e: forward(lax.rem(blk + step, blks), e).wait_recv())
    for e in range(1, halves):
        level_three(lax.rem(half + e, halves) * blks)

    for q in range(groups // OCT):
        pieces = []
        for o in range(OCT):
            lanes = slice(o * width, (o + 1) * width)
            column = q * OCT + o
            box = three[column] * keep3[:, column : column + 1]
            pieces.append(phase[2, :, lanes] * box + phase[3, :, lanes] * pltpu.roll(box, width // 2, 1))
        keep4 = jnp.sum(jnp.where(diagonal, need4[q : q + 1, :].astype(F32), 0.0), 1, keepdims=True)
        four = product(pieces) * keep4
        cone_out[:, q, :] = four[:cones]

    each(blks * subs, lambda d: copy(d).wait_send())
    for step in range(blks):
        each(halves, lambda e: forward(lax.rem(blk + step, blks), e).wait_send())


def put_out(low_ref, cone_ref, low_out, cone_out, sems):
    copies = [
        pltpu.make_async_copy(low_ref, low_out, sems.at[0]),
        pltpu.make_async_copy(cone_ref, cone_out, sems.at[1]),
    ]
    for copy in copies:
        copy.start()
    for copy in copies:
        copy.wait()


def solution(mesh):
    halves, blks, subs = mesh.shape["half"], mesh.shape["blk"], mesh.shape["sub"]
    groups = halves * blks

    def local(leaf, occupied, angles, need3, need4):
        rows, width = leaf.shape
        pairs = rows // (2 * OCT)
        per_sub = pairs // subs
        cones = need3.shape[0]
        padded = -(-cones // 8) * 8
        assert per_sub == OCT and need3.shape[1] == groups
        weight = jnp.asarray(weight_table(ORDER))
        lane = jnp.asarray(lane_table(ORDER))
        occupied = occupied.reshape(rows // 128, 128)
        need4 = need4.T
        vmem = pl.BlockSpec(memory_space=pltpu.VMEM)
        anywhere = pl.BlockSpec(memory_space=pl.ANY)
        results = pl.pallas_call(
            functools.partial(kernel, halves, blks, subs, cones),
            out_shape=(
                pltpu.VMEM((per_sub, width), F32),
                pltpu.VMEM((cones, groups // OCT, width), F32),
            ),
            in_specs=[anywhere] * 7,
            out_specs=(vmem, vmem),
            scratch_shapes=[
                pltpu.VMEM(leaf.shape, F32),
                pltpu.VMEM(occupied.shape, jnp.int32),
                pltpu.VMEM(angles.shape, F32),
                pltpu.VMEM(need3.shape, jnp.int32),
                pltpu.VMEM(need4.shape, jnp.int32),
                pltpu.VMEM(weight.shape, BF16),
                pltpu.VMEM(lane.shape, F32),
                pltpu.VMEM((pairs, width), F32),
                pltpu.VMEM((blks, subs, per_sub, width), F32),
                pltpu.VMEM((groups, per_sub, width), F32),
                pltpu.VMEM((groups, padded, width), F32),
                pltpu.VMEM((4, padded, OCT * width), F32),
                pltpu.SemaphoreType.DMA((7,)),
                pltpu.SemaphoreType.DMA((blks * subs,)),
                pltpu.SemaphoreType.DMA((blks * subs,)),
                pltpu.SemaphoreType.DMA((blks, halves)),
                pltpu.SemaphoreType.DMA((blks, halves)),
            ],
            compiler_params=pltpu.CompilerParams(collective_id=0, has_side_effects=True),
            name="upward",
        )(leaf, occupied, angles, need3, need4, weight, lane)
        results = [pltpu.with_memory_space_constraint(value, pltpu.VMEM) for value in results]
        return pl.pallas_call(
            put_out,
            out_shape=[jax.ShapeDtypeStruct(value.shape, F32) for value in results],
            in_specs=[vmem] * 2,
            out_specs=[pl.BlockSpec(memory_space=pltpu.HBM)] * 2,
            scratch_shapes=[pltpu.SemaphoreType.DMA((2,))],
            name="put_out",
        )(*results)

    return jax.shard_map(
        local,
        mesh=mesh,
        in_specs=(
            P(("half", "blk", "sub"), None),
            P(("half", "blk", "sub")),
            P(),
            P(("half", "blk"), "sub"),
            P(("half", "blk"), "sub"),
        ),
        out_specs=(P(("half", "blk", "sub"), None), P(("half", "blk"), "sub", None)),
        check_vma=False,
    )
```
